32 devices in a mesh: dom: 8 (over y, x, core), shift: 4 (over z).
Axes of the slice: x: 2, y: 2, z: 4, core: 2. Of those that a mesh axis runs over, the one named last changes fastest.
Arguments:
- sources: float32 [32, 32, 16, 128], P('shift', 'dom'), may hold values from -6 to 6
- kappa: float32 [32, 16, 128], P('dom'), may hold values from 0 to 2
- mass: float32 [32, 16, 128], P('dom'), may hold values from 0.25 to 4
- shift_table: float32 [64], replicated, may hold values from 0.5 to 4
- shift_ids: int32 [16], P('shift'), may hold values from 0 to 63
- sketch: bfloat16 [1024, 32, 16, 128], P(None, 'dom'), may hold values from -0.1875 to 0.1875
Outputs:
- solution: float32 [16, 32, 32, 16, 128], P('shift', None, 'dom')
- residual: float32 [16, 32, 32, 16, 128], P('shift', None, 'dom')
The draws below stay inside these ranges and needn't reach their ends.
Inputs may be any that keep to these rules, and one draw needn't show every extreme that they name: `shift_ids`: index into shift_table.
All inputs are finite; a program needn't handle non-finite values.
Results may differ from the reference program's by a relative error of at most 0.0026.
Values sent between devices are 32-bit elements; how exact they have to be, the bound alone decides.
A program may use at most 128 MiB of HBM per device.

```python
import math
import jax
import jax.numpy as jnp
from jax import lax

SK = 1024
SHIFTS = 16
TABLE = 64
NY = 16
NZ = 128
B = 32
NX = 32


def plant(array, stream_key, least, top_value):
    dims = array.shape
    place = [jax.random.randint(jax.random.fold_in(stream_key, axis), (), 0, dims[axis]) for axis in range(len(dims))]
    array = array.at[tuple(place)].set(least)
    longest = dims.index(max(dims))
    place[longest] = (place[longest] + 1) % dims[longest]
    return array.at[tuple(place)].set(top_value)


def block_scale(own_key, shape, cuts, least, largest):
    gain, own = 1.0, jax.random.fold_in(own_key, 6)
    for dim, blocks in cuts:
        steps = jnp.exp(jax.random.uniform(jax.random.fold_in(own, dim), (blocks,), jnp.float32, least / len(cuts), largest / len(cuts)))
        gain = gain * jnp.repeat(steps, shape[dim] // blocks).reshape([-1 if axis == dim else 1 for axis in range(len(shape))])
    return gain


def gaussian(key, shape, deviation, reach, pieces=(), held_as=jnp.bfloat16):
    drawn = jax.random.normal(key, shape, jnp.float32) * deviation
    if len(pieces) > 0:
        drawn = block_scale(key, shape, pieces, -0.22, 0.18) * drawn
    return jnp.clip(drawn, min=-reach, max=reach).astype(held_as)


def setup_inputs(seed: int = 0) -> dict:
    splits = jax.random.split(jax.random.key(seed), 7)
    return {
        "sources": gaussian(splits[0], (B, NX, NY, NZ), 1.0, 6.0, ((0, 4), (1, 8)), jnp.float32),
        "kappa": jnp.clip(2.0 * jax.random.uniform(splits[1], (NX, NY, NZ), jnp.float32) ** block_scale(splits[1], (NX, NY, NZ), ((0, 8),), -0.2, 0.2), 0.0, 2.0),
        "mass": jnp.clip(jnp.exp(math.log(4.0) - 2.7725887 * jax.random.uniform(splits[2], (NX, NY, NZ), jnp.float32) ** block_scale(splits[2], (NX, NY, NZ), ((0, 8),), -0.2, 0.2)), 0.25, 4.0),
        "shift_table": jnp.clip(jax.random.uniform(splits[3], (TABLE,), jnp.float32, 0.5, 4.0), 0.5, 4.0),
        "shift_ids": plant(jax.random.randint(splits[4], (SHIFTS,), 0, TABLE), jax.random.fold_in(splits[4], 1), 0, TABLE - 1).astype(jnp.int32),
        "sketch": gaussian(splits[5], (SK, NX, NY, NZ), SK ** -0.5, 0.1875, ((1, 8),)),
    }


def shift_values(shift_table, shift_ids):
    entries = jnp.arange(shift_table.shape[0], dtype=jnp.int32)
    picked = jnp.where(shift_ids[:, None] == entries[None, :], shift_table[None, :], 0.0)
    return lax.optimization_barrier(jnp.sum(picked, axis=1))

def apply_operator(field, diag):
    padded = jnp.pad(field, ((0, 0), (1, 1), (1, 1), (1, 1)))
    beside = padded[:, 2:, 1:-1, 1:-1] + padded[:, :-2, 1:-1, 1:-1]
    beside = beside + padded[:, 1:-1, 2:, 1:-1] + padded[:, 1:-1, :-2, 1:-1]
    beside = beside + padded[:, 1:-1, 1:-1, 2:] + padded[:, 1:-1, 1:-1, :-2]
    return diag * field - beside

def solve_small(gram):
    h_vals = [gram[:, 1 + i, 0] for i in range(3)]
    ridge = 0.001 * (gram[:, 1, 1] + gram[:, 2, 2] + gram[:, 3, 3]) / 3.0 + 1.0
    entry = [[gram[:, 1 + i, 1 + k] + (ridge if i == k else 0.0) for k in range(3)] for i in range(3)]
    l00 = jnp.sqrt(entry[0][0])
    l10 = entry[1][0] / l00
    l20 = entry[2][0] / l00
    l11 = jnp.sqrt(entry[1][1] - l10 * l10)
    l21 = (entry[2][1] - l20 * l10) / l11
    l22 = jnp.sqrt(entry[2][2] - l20 * l20 - l21 * l21)
    f0 = h_vals[0] / l00
    f1 = (h_vals[1] - l10 * f0) / l11
    f2 = (h_vals[2] - l20 * f0 - l21 * f1) / l22
    c2 = f2 / l22
    c1 = (f1 - l21 * c2) / l11
    c0 = (f0 - l10 * c1 - l20 * c2) / l00
    return (c0, c1, c2)

def gram_of(sketched):
    return jnp.einsum('rib,rkb->bik', sketched, sketched, precision=lax.Precision.HIGHEST)

def reference(sources, kappa, mass, shift_table, shift_ids, sketch):
    sigma = shift_values(shift_table, shift_ids)
    matrix = sketch.reshape(sketch.shape[0], -1)
    count = sources.shape[0]

    def one_shift(value):
        diag = (6.0 - kappa + value * mass)[None]
        center = 6.0 + value
        w0 = sources
        z0 = apply_operator(w0, diag)
        w1 = (z0 - center * w0) / 6.0
        z1 = apply_operator(w1, diag)
        w2 = (z1 - center * w1) / 6.0
        z2 = apply_operator(w2, diag)
        stacked = jnp.stack([w0, z0, z1, z2], axis=0).astype(jnp.bfloat16).reshape(4 * count, -1)
        sketched = lax.dot_general(matrix, stacked, (((1,), (1,)), ((), ())), preferred_element_type=jnp.float32)
        gram = gram_of(sketched.reshape(matrix.shape[0], 4, count))
        c0, c1, c2 = solve_small(gram)
        c0 = c0[:, None, None, None]
        c1 = c1[:, None, None, None]
        c2 = c2[:, None, None, None]
        solution = c0 * w0 + c1 * w1 + c2 * w2
        residual = w0 - c0 * z0 - c1 * z1 - c2 * z2
        return (solution, residual)
    solution, residual = lax.map(one_shift, sigma)
    return (solution, residual)
```

```python
import functools

import jax
import jax.numpy as jnp
from jax import lax
from jax.experimental import pallas as pl
from jax.experimental.pallas import tpu as pltpu
from jax.sharding import PartitionSpec as P

HALO = 3
LANES = 128
MID = 2.25
BASIS = 10
IMAGES = ((1, 2), (3, 4, 5), (6, 7, 8, 9))
PAIRS = [(i, k) for i in range(BASIS) for k in range(i, BASIS)]
PAIR_INDEX = {pair: n for n, pair in enumerate(PAIRS)}


def neighbour_sum(field):
    inner = field[1:-1]
    shape = inner.shape
    total = field[2:] + field[:-2]
    for dim in (1, 2):
        size = shape[dim]
        place = lax.broadcasted_iota(jnp.int32, shape, dim)
        total = total + jnp.where(place > 0, pltpu.roll(inner, 1, dim), 0.0)
        total = total + jnp.where(place < size - 1, pltpu.roll(inner, size - 1, dim), 0.0)
    return total


def plane_mask(shape, width, low, high):
    plane = lax.broadcasted_iota(jnp.int32, shape, 0)
    return jnp.where(plane < width, low, jnp.where(plane >= shape[0] - width, high, 1.0))


def edge_flags():
    me = lax.axis_index("dom")
    last = lax.axis_size("dom") - 1
    return (me > 0).astype(jnp.float32), (me < last).astype(jnp.float32)


def basis_fields(w0, diag, mass, mask1, mask2):
    sixth = 1.0 / 6.0
    center = 6.0 + MID
    d1, m1 = diag[1:-1], mass[1:-1]
    d2, m2 = diag[2:-2], mass[2:-2]
    d3, m3 = diag[3:-3], mass[3:-3]
    w0i = w0[1:-1]
    a0 = d1 * w0i - neighbour_sum(w0)
    a1 = m1 * w0i
    scaled1 = sixth * mask1
    g0 = (a0 - center * w0i) * scaled1
    g1 = (a1 - w0i) * scaled1
    g0i, g1i = g0[1:-1], g1[1:-1]
    b0 = d2 * g0i - neighbour_sum(g0)
    b1 = d2 * g1i - neighbour_sum(g1) + m2 * g0i
    b2 = m2 * g1i
    scaled2 = sixth * mask2
    h0 = (b0 - center * g0i) * scaled2
    h1 = (b1 - center * g1i - g0i) * scaled2
    h2 = (b2 - g1i) * scaled2
    h0i, h1i, h2i = h0[1:-1], h1[1:-1], h2[1:-1]
    e0 = d3 * h0i - neighbour_sum(h0)
    e1 = d3 * h1i - neighbour_sum(h1) + m3 * h0i
    e2 = d3 * h2i - neighbour_sum(h2) + m3 * h1i
    e3 = m3 * h2i
    return [
        w0[3:-3], a0[2:-2], a1[2:-2], b0[1:-1], b1[1:-1], b2[1:-1], e0, e1, e2, e3
    ]


def solve_small(h_vals, entry):
    l00 = jnp.sqrt(entry[0][0])
    l10 = entry[1][0] / l00
    l20 = entry[2][0] / l00
    l11 = jnp.sqrt(entry[1][1] - l10 * l10)
    l21 = (entry[2][1] - l20 * l10) / l11
    l22 = jnp.sqrt(entry[2][2] - l20 * l20 - l21 * l21)
    f0 = h_vals[0] / l00
    f1 = (h_vals[1] - l10 * f0) / l11
    f2 = (h_vals[2] - l20 * f0 - l21 * f1) / l22
    c2 = f2 / l22
    c1 = (f1 - l21 * c2) / l11
    c0 = (f0 - l10 * c1 - l20 * c2) / l00
    return (c0, c1, c2)


def coefficients(gram, tau):
    def product(left, right):
        by_degree = {}
        for p, i in enumerate(left):
            for q, k in enumerate(right):
                n = PAIR_INDEX[(min(i, k), max(i, k))]
                column = gram[:, n : n + 1]
                by_degree[p + q] = by_degree[p + q] + column if p + q in by_degree else column
        top = max(by_degree)
        total = jnp.broadcast_to(by_degree[top], (gram.shape[0], LANES))
        for degree in range(top - 1, -1, -1):
            total = total * tau + by_degree[degree]
        return total

    h_vals = [product(image, (0,)) for image in IMAGES]
    entry = [[None] * 3 for _ in range(3)]
    for i in range(3):
        for k in range(i + 1):
            entry[i][k] = product(IMAGES[i], IMAGES[k])
    ridge = 0.001 * (entry[0][0] + entry[1][1] + entry[2][2]) / 3.0 + 1.0
    for i in range(3):
        entry[i][i] = entry[i][i] + ridge
    return solve_small(h_vals, entry)


def project_kernel(
    n, groups, src_ref, kappa_ref, mass_ref, table_ref, ids_ref, sketch_ref,
    wide_ref, coeff_ref, c_ref,
    rows_buf, raw_ref, fields_ref, out_buf, in_buf, gram_own, gram_in, gram_all,
    load_sem, z_send, z_recv, halo_send, halo_recv, km_send, km_recv,
    rs_send, rs_recv, g_send, g_recv, s_send, s_recv,
):
    me = lax.axis_index("dom")
    group = lax.axis_index("shift")
    nb, slab = src_ref.shape[0], src_ref.shape[1]
    block = rows_buf.shape[1]
    columns = BASIS * nb
    right, left = lax.rem(me + 1, n), lax.rem(me + n - 1, n)
    has_right, has_left = me < n - 1, me > 0

    def remote(src, dst, send, recv, **where):
        return pltpu.make_async_remote_copy(
            src_ref=src, dst_ref=dst, send_sem=send, recv_sem=recv,
            device_id=where, device_id_type=pl.DeviceIdType.MESH,
        )

    def load(t):
        owner = lax.rem(me + 1 + t, n)
        return pltpu.make_async_copy(
            sketch_ref.at[pl.ds(owner * block, block)], rows_buf.at[t], load_sem.at[t]
        )

    barrier = pltpu.get_barrier_semaphore()
    for t in range(1, n):
        pl.semaphore_signal(
            barrier, inc=1, device_id={"dom": lax.rem(me + t, n)},
            device_id_type=pl.DeviceIdType.MESH,
        )
    for t in range(1, groups):
        pl.semaphore_signal(
            barrier, inc=1, device_id={"shift": lax.rem(group + t, groups)},
            device_id_type=pl.DeviceIdType.MESH,
        )
    for t in range(n):
        load(t).start()
    pl.semaphore_wait(barrier, n - 1 + groups - 1)

    def halo(t, side):
        slot = lax.rem(group + groups - t, groups)
        if side == 0:
            planes, target, there = pl.ds(slab - HALO, HALO), pl.ds(0, HALO), right
        else:
            planes, target, there = pl.ds(0, HALO), pl.ds(slab + HALO, HALO), left
        if t == 0:
            src = src_ref.at[:, planes]
        else:
            start = slab if side == 0 else HALO
            src = wide_ref.at[slot, :, pl.ds(start, HALO)]
        return remote(
            src, wide_ref.at[slot, :, target], halo_send.at[t, side], halo_recv.at[t, side],
            dom=there,
        )

    def coeff_halo(which, side):
        ref = (kappa_ref, mass_ref)[which]
        if side == 0:
            planes, target, there = pl.ds(slab - HALO, HALO), pl.ds(0, HALO), right
        else:
            planes, target, there = pl.ds(0, HALO), pl.ds(slab + HALO, HALO), left
        return remote(
            ref.at[planes], coeff_ref.at[which, target], km_send.at[which, side],
            km_recv.at[which, side], dom=there,
        )

    def across(t):
        return remote(
            src_ref, wide_ref.at[group, :, pl.ds(HALO, slab)], z_send.at[t - 1], z_recv.at[t - 1],
            shift=lax.rem(group + t, groups),
        )

    @pl.when(has_right)
    def _():
        halo(0, 0).start()
        for which in range(2):
            coeff_halo(which, 0).start()

    @pl.when(has_left)
    def _():
        halo(0, 1).start()
        for which in range(2):
            coeff_halo(which, 1).start()

    for t in range(1, groups):
        across(t).start()

    wide_ref[group, :, pl.ds(HALO, slab)] = src_ref[...]
    coeff_ref[0, pl.ds(HALO, slab)] = kappa_ref[...]
    coeff_ref[1, pl.ds(HALO, slab)] = mass_ref[...]

    @pl.when(jnp.logical_not(has_left))
    def _():
        wide_ref[:, :, pl.ds(0, HALO)] = jnp.zeros(
            (groups, nb, HALO) + src_ref.shape[2:], jnp.float32
        )
        coeff_ref[:, pl.ds(0, HALO)] = jnp.zeros((2, HALO) + src_ref.shape[2:], jnp.float32)

    @pl.when(jnp.logical_not(has_right))
    def _():
        wide_ref[:, :, pl.ds(slab + HALO, HALO)] = jnp.zeros(
            (groups, nb, HALO) + src_ref.shape[2:], jnp.float32
        )
        coeff_ref[:, pl.ds(slab + HALO, HALO)] = jnp.zeros(
            (2, HALO) + src_ref.shape[2:], jnp.float32
        )

    @pl.when(has_left)
    def _():
        halo(0, 0).wait_recv()
        for which in range(2):
            coeff_halo(which, 0).wait_recv()

    @pl.when(has_right)
    def _():
        halo(0, 1).wait_recv()
        for which in range(2):
            coeff_halo(which, 1).wait_recv()

    low, high = edge_flags()
    mass = coeff_ref[1]
    diag = (6.0 - coeff_ref[0]) + MID * mass
    planes = slab + 2 * HALO
    grid_tail = src_ref.shape[2:]
    mask1 = plane_mask((planes - 2,) + grid_tail, 2, low, high)
    mask2 = plane_mask((planes - 4,) + grid_tail, 1, low, high)

    def one_source(b, carry):
        fields = basis_fields(wide_ref[group, b], diag, mass, mask1, mask2)
        for k, field in enumerate(fields):
            rounded = field.astype(jnp.bfloat16)
            raw_ref[k * nb + b] = rounded
            raw_ref[columns + k * nb + b] = (field - rounded.astype(jnp.float32)).astype(
                jnp.bfloat16
            )
        return carry

    lax.fori_loop(0, nb, one_source, 0)
    fields_ref[...] = raw_ref[...].reshape(fields_ref.shape)

    def forward(t):
        across(t).wait_recv()

        @pl.when(has_right)
        def _():
            halo(t, 0).start()

        @pl.when(has_left)
        def _():
            halo(t, 1).start()

    def scatter(t):
        return remote(
            out_buf.at[t], in_buf.at[t], rs_send.at[t], rs_recv.at[t],
            dom=lax.rem(me + 1 + t, n),
        )

    def multiply(t):
        load(t).wait()
        product = lax.dot_general(
            rows_buf[t].reshape(block, fields_ref.shape[1]), fields_ref[...],
            (((1,), (1,)), ((), ())), preferred_element_type=jnp.float32,
        )
        turned = product.T
        return turned[:columns] + turned[columns:]

    def step(t, carry):
        out_buf[t] = multiply(t)
        scatter(t).start()
        return carry

    lax.fori_loop(0, n - 1, step, 0)
    total = multiply(n - 1)
    for t in range(1, groups):
        forward(t)

    for t in range(n - 1):
        scatter(t).wait_recv()
        total = total + in_buf[t]

    lane = lax.broadcasted_iota(jnp.int32, (nb, LANES), 1)
    gram = jnp.zeros((nb, LANES), jnp.float32)
    for p, (i, k) in enumerate(PAIRS):
        value = jnp.sum(
            total[i * nb : (i + 1) * nb] * total[k * nb : (k + 1) * nb], axis=1, keepdims=True
        )
        gram = jnp.where(lane == p, value, gram)
    gram_own[...] = gram

    def share(t):
        return remote(
            gram_own, gram_in.at[t - 1], g_send.at[t - 1], g_recv.at[t - 1],
            dom=lax.rem(me + t, n),
        )

    for t in range(1, n):
        share(t).start()
    for t in range(1, n):
        share(t).wait_recv()
        gram = gram + gram_in[t - 1]
    gram_all[group] = gram

    def spread(t):
        return remote(
            gram_all.at[group], gram_all.at[group], s_send.at[t - 1], s_recv.at[t - 1],
            shift=lax.rem(group + t, groups),
        )

    for t in range(1, groups):
        spread(t).start()
    tau = jnp.zeros((1, LANES), jnp.float32)
    lane_row = lax.broadcasted_iota(jnp.int32, (1, LANES), 1)
    for j in range(ids_ref.shape[0]):
        tau = jnp.where(lane_row == j, table_ref[ids_ref[j]] - MID, tau)
    for t in range(1, groups):
        spread(t).wait_recv()
    count = groups * nb
    solved = coefficients(gram_all[...].reshape(count, LANES), tau)
    for i in range(3):
        c_ref[pl.ds(i * count, count)] = solved[i]

    for t in range(1, groups):
        @pl.when(has_left)
        def _():
            halo(t, 0).wait_recv()

        @pl.when(has_right)
        def _():
            halo(t, 1).wait_recv()

    @pl.when(has_right)
    def _():
        for t in range(groups):
            halo(t, 0).wait_send()
        for which in range(2):
            coeff_halo(which, 0).wait_send()

    @pl.when(has_left)
    def _():
        for t in range(groups):
            halo(t, 1).wait_send()
        for which in range(2):
            coeff_halo(which, 1).wait_send()

    for t in range(1, groups):
        across(t).wait_send()
        spread(t).wait_send()
    for t in range(n - 1):
        scatter(t).wait_send()
    for t in range(1, n):
        share(t).wait_send()


def combine_kernel(count, wide_ref, coeff_ref, c_ref, table_ref, ids_ref, sol_ref, res_ref):
    batch, planes = wide_ref.shape[0], wide_ref.shape[1]
    grid_tail = wide_ref.shape[2:]
    low, high = edge_flags()
    sixth = 1.0 / 6.0
    scaled1 = sixth * plane_mask((planes - 2,) + grid_tail, 2, low, high)
    scaled2 = sixth * plane_mask((planes - 4,) + grid_tail, 1, low, high)
    first = pl.program_id(0) * batch

    def one_source(i, carry):
        w0 = wide_ref[i]
        w0i = w0[1:-1]
        own = w0[3:-3]
        base = (6.0 - coeff_ref[0, 1:-1])
        near = neighbour_sum(w0)
        for j in range(ids_ref.shape[0]):
            sigma = table_ref[ids_ref[j]]
            center = 6.0 + sigma
            diag = base + sigma * coeff_ref[1, 1:-1]
            z0 = diag * w0i - near
            w1 = (z0 - center * w0i) * scaled1
            w1i = w1[1:-1]
            z1 = diag[1:-1] * w1i - neighbour_sum(w1)
            w2 = (z1 - center * w1i) * scaled2
            w2i = w2[1:-1]
            z2 = diag[2:-2] * w2i - neighbour_sum(w2)
            b = first + i
            c0 = c_ref[b, j]
            c1 = c_ref[count + b, j]
            c2 = c_ref[2 * count + b, j]
            sol_ref[j, i] = c0 * own + c1 * w1[2:-2] + c2 * w2i
            res_ref[j, i] = own - c0 * z0[2:-2] - c1 * z1[1:-1] - c2 * z2
        return carry

    lax.fori_loop(0, batch, one_source, 0)


def on_device(sources, kappa, mass, shift_table, shift_ids, sketch):
    n, groups = lax.axis_size("dom"), lax.axis_size("shift")
    nb, slab = sources.shape[0], sources.shape[1]
    tail = sources.shape[2:]
    shifts = shift_ids.shape[0]
    rows = sketch.shape[0]
    block = rows // n
    cells = slab * tail[0] * tail[1]
    planes = slab + 2 * HALO
    count = groups * nb
    columns = BASIS * nb
    vmem = pl.BlockSpec(memory_space=pltpu.VMEM)
    smem = pl.BlockSpec(memory_space=pltpu.SMEM)
    dma = pltpu.SemaphoreType.DMA
    f32 = jnp.float32
    wide, coeff, solved = pl.pallas_call(
        functools.partial(project_kernel, n, groups),
        out_shape=(
            jax.ShapeDtypeStruct((groups, nb, planes) + tail, f32),
            jax.ShapeDtypeStruct((2, planes) + tail, f32),
            jax.ShapeDtypeStruct((3 * count, LANES), f32),
        ),
        in_specs=[vmem, vmem, vmem, smem, smem, pl.BlockSpec(memory_space=pl.ANY)],
        out_specs=(vmem, vmem, vmem),
        scratch_shapes=[
            pltpu.VMEM((n, block, slab) + tail, jnp.bfloat16),
            pltpu.VMEM((2 * columns, slab) + tail, jnp.bfloat16),
            pltpu.VMEM((2 * columns, cells), jnp.bfloat16),
            pltpu.VMEM((n - 1, columns, block), f32),
            pltpu.VMEM((n - 1, columns, block), f32),
            pltpu.VMEM((nb, LANES), f32),
            pltpu.VMEM((n - 1, nb, LANES), f32),
            pltpu.VMEM((groups, nb, LANES), f32),
            dma((n,)),
            dma((groups - 1,)), dma((groups - 1,)),
            dma((groups, 2)), dma((groups, 2)),
            dma((2, 2)), dma((2, 2)),
            dma((n - 1,)), dma((n - 1,)),
            dma((n - 1,)), dma((n - 1,)),
            dma((groups - 1,)), dma((groups - 1,)),
        ],
        compiler_params=pltpu.CompilerParams(
            collective_id=0, has_side_effects=True, vmem_limit_bytes=56 << 20
        ),
        name="project",
    )(sources, kappa, mass, shift_table, shift_ids, sketch)

    batch = 4 if count % 4 == 0 else 1
    out = jax.ShapeDtypeStruct((shifts, count, slab) + tail, f32)
    out_spec = pl.BlockSpec((shifts, batch, slab) + tail, lambda i: (0, i, 0, 0, 0))
    return pl.pallas_call(
        functools.partial(combine_kernel, count),
        grid=(count // batch,),
        out_shape=(out, out),
        in_specs=[
            pl.BlockSpec((batch, planes) + tail, lambda i: (i, 0, 0, 0)),
            pl.BlockSpec((2, planes) + tail, lambda i: (0, 0, 0, 0)),
            smem, smem, smem,
        ],
        out_specs=(out_spec, out_spec),
        compiler_params=pltpu.CompilerParams(vmem_limit_bytes=32 << 20),
        name="combine",
    )(wide.reshape((count, planes) + tail), coeff, solved, shift_table, shift_ids)


def solution(mesh):
    placed = (
        P("shift", "dom", None, None),
        P("dom", None, None),
        P("dom", None, None),
        P(),
        P("shift"),
        P(None, "dom", None, None),
    )
    return jax.shard_map(
        on_device,
        mesh=mesh,
        in_specs=placed,
        out_specs=(P("shift", None, "dom", None, None), P("shift", None, "dom", None, None)),
        check_vma=False,
    )
```

```python
import functools

import jax
import jax.numpy as jnp
from jax import lax
from jax.experimental import pallas as pl
from jax.experimental.pallas import tpu as pltpu
from jax.sharding import PartitionSpec as P

HALO = 3
LANES = 128
MID = 2.25
BASIS = 10
IMAGES = ((1, 2), (3, 4, 5), (6, 7, 8, 9))
PAIRS = [(i, k) for i in range(BASIS) for k in range(i, BASIS)]
PAIR_INDEX = {pair: n for n, pair in enumerate(PAIRS)}


def neighbour_sum(field):
    inner = field[1:-1]
    shape = inner.shape
    total = field[2:] + field[:-2]
    for dim in (1, 2):
        size = shape[dim]
        place = lax.broadcasted_iota(jnp.int32, shape, dim)
        total = total + jnp.where(place > 0, pltpu.roll(inner, 1, dim), 0.0)
        total = total + jnp.where(place < size - 1, pltpu.roll(inner, size - 1, dim), 0.0)
    return total


def plane_mask(shape, width, low, high):
    plane = lax.broadcasted_iota(jnp.int32, shape, 0)
    return jnp.where(plane < width, low, jnp.where(plane >= shape[0] - width, high, 1.0))


def edge_flags():
    me = lax.axis_index("dom")
    last = lax.axis_size("dom") - 1
    return (me > 0).astype(jnp.float32), (me < last).astype(jnp.float32)


def basis_fields(w0, diag, mass, mask1, mask2):
    sixth = 1.0 / 6.0
    center = 6.0 + MID
    d1, m1 = diag[1:-1], mass[1:-1]
    d2, m2 = diag[2:-2], mass[2:-2]
    d3, m3 = diag[3:-3], mass[3:-3]
    w0i = w0[1:-1]
    a0 = d1 * w0i - neighbour_sum(w0)
    a1 = m1 * w0i
    scaled1 = sixth * mask1
    g0 = (a0 - center * w0i) * scaled1
    g1 = (a1 - w0i) * scaled1
    g0i, g1i = g0[1:-1], g1[1:-1]
    b0 = d2 * g0i - neighbour_sum(g0)
    b1 = d2 * g1i - neighbour_sum(g1) + m2 * g0i
    b2 = m2 * g1i
    scaled2 = sixth * mask2
    h0 = (b0 - center * g0i) * scaled2
    h1 = (b1 - center * g1i - g0i) * scaled2
    h2 = (b2 - g1i) * scaled2
    h0i, h1i, h2i = h0[1:-1], h1[1:-1], h2[1:-1]
    e0 = d3 * h0i - neighbour_sum(h0)
    e1 = d3 * h1i - neighbour_sum(h1) + m3 * h0i
    e2 = d3 * h2i - neighbour_sum(h2) + m3 * h1i
    e3 = m3 * h2i
    return [
        w0[3:-3], a0[2:-2], a1[2:-2], b0[1:-1], b1[1:-1], b2[1:-1], e0, e1, e2, e3
    ]


def solve_small(h_vals, entry):
    l00 = jnp.sqrt(entry[0][0])
    l10 = entry[1][0] / l00
    l20 = entry[2][0] / l00
    l11 = jnp.sqrt(entry[1][1] - l10 * l10)
    l21 = (entry[2][1] - l20 * l10) / l11
    l22 = jnp.sqrt(entry[2][2] - l20 * l20 - l21 * l21)
    f0 = h_vals[0] / l00
    f1 = (h_vals[1] - l10 * f0) / l11
    f2 = (h_vals[2] - l20 * f0 - l21 * f1) / l22
    c2 = f2 / l22
    c1 = (f1 - l21 * c2) / l11
    c0 = (f0 - l10 * c1 - l20 * c2) / l00
    return (c0, c1, c2)


def coefficients(gram, tau):
    def product(left, right):
        by_degree = {}
        for p, i in enumerate(left):
            for q, k in enumerate(right):
                n = PAIR_INDEX[(min(i, k), max(i, k))]
                column = gram[:, n : n + 1]
                by_degree[p + q] = by_degree[p + q] + column if p + q in by_degree else column
        top = max(by_degree)
        total = jnp.broadcast_to(by_degree[top], (gram.shape[0], LANES))
        for degree in range(top - 1, -1, -1):
            total = total * tau + by_degree[degree]
        return total

    h_vals = [product(image, (0,)) for image in IMAGES]
    entry = [[None] * 3 for _ in range(3)]
    for i in range(3):
        for k in range(i + 1):
            entry[i][k] = product(IMAGES[i], IMAGES[k])
    ridge = 0.001 * (entry[0][0] + entry[1][1] + entry[2][2]) / 3.0 + 1.0
    for i in range(3):
        entry[i][i] = entry[i][i] + ridge
    return solve_small(h_vals, entry)


def project_kernel(
    n, groups, src_hbm, kappa_hbm, mass_hbm, table_ref, ids_ref, sketch_ref,
    wide_ref, coeff_ref, c_ref,
    src_ref, kappa_ref, mass_ref, mine_ref, rows_buf, raw_ref, fields_ref, out_buf, in_buf, gram_own, gram_in, gram_all,
    load_sem, in_sem, own_sem, own_send, own_recv, z_send, z_recv, halo_send, halo_recv, km_send, km_recv,
    rs_send, rs_recv, g_send, g_recv, s_send, s_recv,
):
    me = lax.axis_index("dom")
    group = lax.axis_index("shift")
    nb, slab = src_ref.shape[0], src_ref.shape[1]
    block = rows_buf.shape[1]
    columns = BASIS * nb
    right, left = lax.rem(me + 1, n), lax.rem(me + n - 1, n)
    has_right, has_left = me < n - 1, me > 0

    def remote(src, dst, send, recv, **where):
        return pltpu.make_async_remote_copy(
            src_ref=src, dst_ref=dst, send_sem=send, recv_sem=recv,
            device_id=where, device_id_type=pl.DeviceIdType.MESH,
        )

    def load(t):
        owner = lax.rem(me + 1 + t, n)
        return pltpu.make_async_copy(
            sketch_ref.at[pl.ds(owner * block, block)], rows_buf.at[t], load_sem.at[t]
        )

    barrier = pltpu.get_barrier_semaphore()
    for t in range(1, n):
        pl.semaphore_signal(
            barrier, inc=1, device_id={"dom": lax.rem(me + t, n)},
            device_id_type=pl.DeviceIdType.MESH,
        )
    for t in range(1, groups):
        pl.semaphore_signal(
            barrier, inc=1, device_id={"shift": lax.rem(group + t, groups)},
            device_id_type=pl.DeviceIdType.MESH,
        )
    arguments = [
        pltpu.make_async_copy(src_hbm, src_ref, in_sem.at[0]),
        pltpu.make_async_copy(kappa_hbm, kappa_ref, in_sem.at[1]),
        pltpu.make_async_copy(mass_hbm, mass_ref, in_sem.at[2]),
    ]
    for copy in arguments:
        copy.start()
    for t in range(n):
        load(t).start()
    for copy in arguments:
        copy.wait()
    pl.semaphore_wait(barrier, n - 1 + groups - 1)

    def sides(side):
        if side == 0:
            return slab - HALO, pl.ds(0, HALO), right
        return 0, pl.ds(slab + HALO, HALO), left

    def own_halo(side):
        first, target, there = sides(side)
        return remote(
            src_ref.at[:, pl.ds(first, HALO)], mine_ref.at[:, target],
            own_send.at[side], own_recv.at[side], dom=there,
        )

    hops = []
    for k in range(1, groups // 2 + 1):
        for way in range(2):
            parts = (0, nb)
            if 2 * k == groups:
                parts = ((0, nb // 2), (nb // 2, nb - nb // 2))[way]
            hops.append((way, k, pl.ds(*parts)))

    def shifted(way, k):
        step = k if way == 0 else groups - k
        return lax.rem(group + step, groups)

    def across(hop):
        way, k, part = hop
        if k == 1:
            slot, src = group, src_ref.at[part]
        else:
            slot = shifted(1 - way, k - 1)
            src = wide_ref.at[slot, part, pl.ds(HALO, slab)]
        return remote(
            src, wide_ref.at[slot, part, pl.ds(HALO, slab)],
            z_send.at[way, k - 1], z_recv.at[way, k - 1], shift=shifted(way, 1),
        )

    def halo(hop, side):
        way, k, part = hop
        slot = shifted(1 - way, k)
        first, target, there = sides(side)
        return remote(
            wide_ref.at[slot, part, pl.ds(HALO + first, HALO)], wide_ref.at[slot, part, target],
            halo_send.at[way, k - 1, side], halo_recv.at[way, k - 1, side], dom=there,
        )

    def coeff_halo(which, side):
        ref = (kappa_ref, mass_ref)[which]
        first, target, there = sides(side)
        return remote(
            ref.at[pl.ds(first, HALO)], coeff_ref.at[which, target], km_send.at[which, side],
            km_recv.at[which, side], dom=there,
        )

    @pl.when(has_right)
    def _():
        own_halo(0).start()
        for which in range(2):
            coeff_halo(which, 0).start()

    @pl.when(has_left)
    def _():
        own_halo(1).start()
        for which in range(2):
            coeff_halo(which, 1).start()

    for hop in hops:
        if hop[1] == 1:
            across(hop).start()

    mine_ref[:, pl.ds(HALO, slab)] = src_ref[...]
    coeff_ref[0, pl.ds(HALO, slab)] = kappa_ref[...]
    coeff_ref[1, pl.ds(HALO, slab)] = mass_ref[...]

    @pl.when(jnp.logical_not(has_left))
    def _():
        mine_ref[:, pl.ds(0, HALO)] = jnp.zeros(
            (nb, HALO) + src_ref.shape[2:], jnp.float32
        )
        coeff_ref[:, pl.ds(0, HALO)] = jnp.zeros((2, HALO) + src_ref.shape[2:], jnp.float32)

    @pl.when(jnp.logical_not(has_right))
    def _():
        mine_ref[:, pl.ds(slab + HALO, HALO)] = jnp.zeros(
            (nb, HALO) + src_ref.shape[2:], jnp.float32
        )
        coeff_ref[:, pl.ds(slab + HALO, HALO)] = jnp.zeros(
            (2, HALO) + src_ref.shape[2:], jnp.float32
        )

    @pl.when(has_left)
    def _():
        own_halo(0).wait_recv()
        for which in range(2):
            coeff_halo(which, 0).wait_recv()

    @pl.when(has_right)
    def _():
        own_halo(1).wait_recv()
        for which in range(2):
            coeff_halo(which, 1).wait_recv()

    keep = pltpu.make_async_copy(mine_ref, wide_ref.at[group], own_sem)
    keep.start()
    low, high = edge_flags()
    mass = coeff_ref[1]
    diag = (6.0 - coeff_ref[0]) + MID * mass
    planes = slab + 2 * HALO
    grid_tail = src_ref.shape[2:]
    mask1 = plane_mask((planes - 2,) + grid_tail, 2, low, high)
    mask2 = plane_mask((planes - 4,) + grid_tail, 1, low, high)

    def one_source(b, carry):
        fields = basis_fields(mine_ref[b], diag, mass, mask1, mask2)
        for k, field in enumerate(fields):
            rounded = field.astype(jnp.bfloat16)
            raw_ref[k * nb + b] = rounded
            raw_ref[columns + k * nb + b] = (field - rounded.astype(jnp.float32)).astype(
                jnp.bfloat16
            )
        return carry

    lax.fori_loop(0, nb, one_source, 0)
    fields_ref[...] = raw_ref[...].reshape(fields_ref.shape)

    def forward(hop):
        across(hop).wait_recv()
        for later in hops:
            if later[0] == hop[0] and later[1] == hop[1] + 1:
                across(later).start()

        @pl.when(has_right)
        def _():
            halo(hop, 0).start()

        @pl.when(has_left)
        def _():
            halo(hop, 1).start()

    early = [hop for hop in hops if hop[1] < groups // 2]
    late = [hop for hop in hops if hop[1] == groups // 2]
    for hop in early:
        forward(hop)

    def scatter(t):
        return remote(
            out_buf.at[t], in_buf.at[t], rs_send.at[t], rs_recv.at[t],
            dom=lax.rem(me + 1 + t, n),
        )

    def multiply(t):
        load(t).wait()
        product = lax.dot_general(
            rows_buf[t].reshape(block, fields_ref.shape[1]), fields_ref[...],
            (((1,), (1,)), ((), ())), preferred_element_type=jnp.float32,
        )
        turned = product.T
        return turned[:columns] + turned[columns:]

    def step(t, carry):
        out_buf[t] = multiply(t)
        scatter(t).start()
        return carry

    lax.fori_loop(0, n - 1, step, 0)
    total = multiply(n - 1)
    for hop in late:
        forward(hop)

    for t in range(n - 1):
        scatter(t).wait_recv()
        total = total + in_buf[t]

    lane = lax.broadcasted_iota(jnp.int32, (nb, LANES), 1)
    gram = jnp.zeros((nb, LANES), jnp.float32)
    for p, (i, k) in enumerate(PAIRS):
        value = jnp.sum(
            total[i * nb : (i + 1) * nb] * total[k * nb : (k + 1) * nb], axis=1, keepdims=True
        )
        gram = jnp.where(lane == p, value, gram)
    gram_own[...] = gram

    def share(t):
        return remote(
            gram_own, gram_in.at[t - 1], g_send.at[t - 1], g_recv.at[t - 1],
            dom=lax.rem(me + t, n),
        )

    for t in range(1, n):
        share(t).start()
    for t in range(1, n):
        share(t).wait_recv()
        gram = gram + gram_in[t - 1]
    gram_all[group] = gram

    def spread(t):
        return remote(
            gram_all.at[group], gram_all.at[group], s_send.at[t - 1], s_recv.at[t - 1],
            shift=lax.rem(group + t, groups),
        )

    for t in range(1, groups):
        spread(t).start()
    tau = jnp.zeros((1, LANES), jnp.float32)
    lane_row = lax.broadcasted_iota(jnp.int32, (1, LANES), 1)
    for j in range(ids_ref.shape[0]):
        tau = jnp.where(lane_row == j, table_ref[ids_ref[j]] - MID, tau)
    for t in range(1, groups):
        spread(t).wait_recv()
    count = groups * nb
    solved = coefficients(gram_all[...].reshape(count, LANES), tau)
    shifts = ids_ref.shape[0]
    packed = jnp.zeros((count, LANES), jnp.float32)
    lane_count = lax.broadcasted_iota(jnp.int32, (count, LANES), 1)
    for i in range(3):
        value = jnp.where(lane_count < shifts, solved[i], 0.0)
        packed = packed + (pltpu.roll(value, i * shifts, 1) if i else value)
    c_ref[...] = packed

    for hop in hops:
        @pl.when(has_left)
        def _():
            halo(hop, 0).wait_recv()

        @pl.when(has_right)
        def _():
            halo(hop, 1).wait_recv()

    keep.wait()

    @pl.when(has_right)
    def _():
        own_halo(0).wait_send()
        for hop in hops:
            halo(hop, 0).wait_send()
        for which in range(2):
            coeff_halo(which, 0).wait_send()

    @pl.when(has_left)
    def _():
        own_halo(1).wait_send()
        for hop in hops:
            halo(hop, 1).wait_send()
        for which in range(2):
            coeff_halo(which, 1).wait_send()

    for t in range(1, groups):
        spread(t).wait_send()
    for hop in hops:
        across(hop).wait_send()
    for t in range(n - 1):
        scatter(t).wait_send()
    for t in range(1, n):
        share(t).wait_send()


def combine_kernel(wide_ref, coeff_ref, c_ref, table_ref, ids_ref, sol_ref, res_ref, step_ref):
    batch, planes = wide_ref.shape[0], wide_ref.shape[1]
    me = lax.axis_index("dom")
    has_low, has_high = me > 0, me < lax.axis_size("dom") - 1
    shifts = ids_ref.shape[0]
    first = pl.program_id(0) * batch

    def inside(field, width):
        return jnp.concatenate(
            [
                jnp.where(has_low, field[:width], 0.0),
                field[width:-width],
                jnp.where(has_high, field[-width:], 0.0),
            ],
            axis=0,
        )

    @pl.when(pl.program_id(0) == 0)
    def _():
        for j in range(shifts):
            sigma = table_ref[ids_ref[j]]
            step_ref[j] = sigma * (coeff_ref[1, 1:-1] - 1.0) - coeff_ref[0, 1:-1]

    def one_source(i, carry):
        w0 = inside(wide_ref[i], HALO)
        own = w0[3:-3]
        near = neighbour_sum(w0)
        b = first + i
        for j in range(shifts):
            center = 6.0 + table_ref[ids_ref[j]]
            v1 = inside(step_ref[j] * w0[1:-1] - near, 2)
            v2 = inside(step_ref[j, 1:-1] * v1[1:-1] - neighbour_sum(v1), 1)
            v3 = step_ref[j, 2:-2] * v2[1:-1] - neighbour_sum(v2)
            v1, v2 = v1[2:-2], v2[1:-1]
            c0 = c_ref[b, j]
            c1 = c_ref[b, shifts + j] * (1.0 / 6.0)
            c2 = c_ref[b, 2 * shifts + j] * (1.0 / 36.0)
            sol_ref[j, i] = c0 * own + c1 * v1 + c2 * v2
            res_ref[j, i] = (
                (1.0 - c0 * center) * own - (c0 + c1 * center) * v1
                - (c1 + c2 * center) * v2 - c2 * v3
            )
        return carry

    lax.fori_loop(0, batch, one_source, 0)


def on_device(sources, kappa, mass, shift_table, shift_ids, sketch):
    n, groups = lax.axis_size("dom"), lax.axis_size("shift")
    nb, slab = sources.shape[0], sources.shape[1]
    tail = sources.shape[2:]
    shifts = shift_ids.shape[0]
    rows = sketch.shape[0]
    block = rows // n
    cells = slab * tail[0] * tail[1]
    planes = slab + 2 * HALO
    count = groups * nb
    columns = BASIS * nb
    vmem = pl.BlockSpec(memory_space=pltpu.VMEM)
    hbm = pl.BlockSpec(memory_space=pl.ANY)
    smem = pl.BlockSpec(memory_space=pltpu.SMEM)
    dma = pltpu.SemaphoreType.DMA
    f32 = jnp.float32
    wide, coeff, solved = pl.pallas_call(
        functools.partial(project_kernel, n, groups),
        out_shape=(
            jax.ShapeDtypeStruct((groups, nb, planes) + tail, f32),
            jax.ShapeDtypeStruct((2, planes) + tail, f32),
            jax.ShapeDtypeStruct((count, LANES), f32),
        ),
        in_specs=[hbm, hbm, hbm, smem, smem, hbm],
        out_specs=(hbm, vmem, vmem),
        scratch_shapes=[
            pltpu.VMEM(sources.shape, f32),
            pltpu.VMEM(kappa.shape, f32),
            pltpu.VMEM(mass.shape, f32),
            pltpu.VMEM((nb, planes) + tail, f32),
            pltpu.VMEM((n, block, slab) + tail, jnp.bfloat16),
            pltpu.VMEM((2 * columns, slab) + tail, jnp.bfloat16),
            pltpu.VMEM((2 * columns, cells), jnp.bfloat16),
            pltpu.VMEM((n - 1, columns, block), f32),
            pltpu.VMEM((n - 1, columns, block), f32),
            pltpu.VMEM((nb, LANES), f32),
            pltpu.VMEM((n - 1, nb, LANES), f32),
            pltpu.VMEM((groups, nb, LANES), f32),
            dma((n,)),
            dma((3,)), dma,
            dma((2,)), dma((2,)),
            dma((2, groups // 2)), dma((2, groups // 2)),
            dma((2, groups // 2, 2)), dma((2, groups // 2, 2)),
            dma((2, 2)), dma((2, 2)),
            dma((n - 1,)), dma((n - 1,)),
            dma((n - 1,)), dma((n - 1,)),
            dma((groups - 1,)), dma((groups - 1,)),
        ],
        compiler_params=pltpu.CompilerParams(
            collective_id=0, has_side_effects=True, vmem_limit_bytes=56 << 20
        ),
        name="project",
    )(sources, kappa, mass, shift_table, shift_ids, sketch)

    batch = 4 if count % 4 == 0 else 1
    out = jax.ShapeDtypeStruct((shifts, count, slab) + tail, f32)
    out_spec = pl.BlockSpec((shifts, batch, slab) + tail, lambda i: (0, i, 0, 0, 0))
    return pl.pallas_call(
        combine_kernel,
        grid=(count // batch,),
        out_shape=(out, out),
        in_specs=[
            pl.BlockSpec((batch, planes) + tail, lambda i: (i, 0, 0, 0)),
            pl.BlockSpec((2, planes) + tail, lambda i: (0, 0, 0, 0)),
            smem, smem, smem,
        ],
        out_specs=(out_spec, out_spec),
        scratch_shapes=[pltpu.VMEM((shifts, planes - 2) + tail, f32)],
        compiler_params=pltpu.CompilerParams(vmem_limit_bytes=32 << 20),
        name="combine",
    )(wide.reshape((count, planes) + tail), coeff, solved, shift_table, shift_ids)


def solution(mesh):
    placed = (
        P("shift", "dom", None, None),
        P("dom", None, None),
        P("dom", None, None),
        P(),
        P("shift"),
        P(None, "dom", None, None),
    )
    return jax.shard_map(
        on_device,
        mesh=mesh,
        in_specs=placed,
        out_specs=(P("shift", None, "dom", None, None), P("shift", None, "dom", None, None)),
        check_vma=False,
    )
```

```python
import functools

import jax
import jax.numpy as jnp
from jax import lax
from jax.experimental import pallas as pl
from jax.experimental.pallas import tpu as pltpu
from jax.sharding import PartitionSpec as P

HALO = 3
PIECES = 2
LANES = 128
MID = 2.25
BASIS = 10
IMAGES = ((1, 2), (3, 4, 5), (6, 7, 8, 9))
PAIRS = [(i, k) for i in range(BASIS) for k in range(i, BASIS)]
PAIR_INDEX = {pair: n for n, pair in enumerate(PAIRS)}


def neighbour_sum(field):
    inner = field[1:-1]
    shape = inner.shape
    total = field[2:] + field[:-2]
    for dim in (1, 2):
        size = shape[dim]
        place = lax.broadcasted_iota(jnp.int32, shape, dim)
        total = total + jnp.where(place > 0, pltpu.roll(inner, 1, dim), 0.0)
        total = total + jnp.where(place < size - 1, pltpu.roll(inner, size - 1, dim), 0.0)
    return total


def plane_mask(shape, width, low, high):
    plane = lax.broadcasted_iota(jnp.int32, shape, 0)
    return jnp.where(plane < width, low, jnp.where(plane >= shape[0] - width, high, 1.0))


def edge_flags():
    me = lax.axis_index("dom")
    last = lax.axis_size("dom") - 1
    return (me > 0).astype(jnp.float32), (me < last).astype(jnp.float32)


def basis_fields(w0, diag, mass, mask1, mask2):
    sixth = 1.0 / 6.0
    center = 6.0 + MID
    d1, m1 = diag[1:-1], mass[1:-1]
    d2, m2 = diag[2:-2], mass[2:-2]
    d3, m3 = diag[3:-3], mass[3:-3]
    w0i = w0[1:-1]
    a0 = d1 * w0i - neighbour_sum(w0)
    a1 = m1 * w0i
    scaled1 = sixth * mask1
    g0 = (a0 - center * w0i) * scaled1
    g1 = (a1 - w0i) * scaled1
    g0i, g1i = g0[1:-1], g1[1:-1]
    b0 = d2 * g0i - neighbour_sum(g0)
    b1 = d2 * g1i - neighbour_sum(g1) + m2 * g0i
    b2 = m2 * g1i
    scaled2 = sixth * mask2
    h0 = (b0 - center * g0i) * scaled2
    h1 = (b1 - center * g1i - g0i) * scaled2
    h2 = (b2 - g1i) * scaled2
    h0i, h1i, h2i = h0[1:-1], h1[1:-1], h2[1:-1]
    e0 = d3 * h0i - neighbour_sum(h0)
    e1 = d3 * h1i - neighbour_sum(h1) + m3 * h0i
    e2 = d3 * h2i - neighbour_sum(h2) + m3 * h1i
    e3 = m3 * h2i
    return [
        w0[3:-3], a0[2:-2], a1[2:-2], b0[1:-1], b1[1:-1], b2[1:-1], e0, e1, e2, e3
    ]


def solve_small(h_vals, entry):
    l00 = jnp.sqrt(entry[0][0])
    l10 = entry[1][0] / l00
    l20 = entry[2][0] / l00
    l11 = jnp.sqrt(entry[1][1] - l10 * l10)
    l21 = (entry[2][1] - l20 * l10) / l11
    l22 = jnp.sqrt(entry[2][2] - l20 * l20 - l21 * l21)
    f0 = h_vals[0] / l00
    f1 = (h_vals[1] - l10 * f0) / l11
    f2 = (h_vals[2] - l20 * f0 - l21 * f1) / l22
    c2 = f2 / l22
    c1 = (f1 - l21 * c2) / l11
    c0 = (f0 - l10 * c1 - l20 * c2) / l00
    return (c0, c1, c2)


def coefficients(gram, tau):
    def product(left, right):
        by_degree = {}
        for p, i in enumerate(left):
            for q, k in enumerate(right):
                n = PAIR_INDEX[(min(i, k), max(i, k))]
                column = gram[:, n : n + 1]
                by_degree[p + q] = by_degree[p + q] + column if p + q in by_degree else column
        top = max(by_degree)
        total = jnp.broadcast_to(by_degree[top], (gram.shape[0], LANES))
        for degree in range(top - 1, -1, -1):
            total = total * tau + by_degree[degree]
        return total

    h_vals = [product(image, (0,)) for image in IMAGES]
    entry = [[None] * 3 for _ in range(3)]
    for i in range(3):
        for k in range(i + 1):
            entry[i][k] = product(IMAGES[i], IMAGES[k])
    ridge = 0.001 * (entry[0][0] + entry[1][1] + entry[2][2]) / 3.0 + 1.0
    for i in range(3):
        entry[i][i] = entry[i][i] + ridge
    return solve_small(h_vals, entry)


def project_kernel(
    n, groups, src_hbm, kappa_hbm, mass_hbm, table_ref, ids_ref, sketch_ref,
    wide_ref, coeff_ref, c_ref,
    src_ref, kappa_ref, mass_ref, mine_ref, rows_buf, raw_ref, fields_ref, out_buf, in_buf, gram_own, gram_in, gram_all,
    load_sem, in_sem, own_sem, own_send, own_recv, z_send, z_recv, halo_send, halo_recv, km_send, km_recv,
    rs_send, rs_recv, g_send, g_recv, s_send, s_recv,
):
    me = lax.axis_index("dom")
    group = lax.axis_index("shift")
    nb, slab = src_ref.shape[0], src_ref.shape[1]
    block = rows_buf.shape[1]
    columns = BASIS * nb
    right, left = lax.rem(me + 1, n), lax.rem(me + n - 1, n)
    has_right, has_left = me < n - 1, me > 0

    def remote(src, dst, send, recv, **where):
        return pltpu.make_async_remote_copy(
            src_ref=src, dst_ref=dst, send_sem=send, recv_sem=recv,
            device_id=where, device_id_type=pl.DeviceIdType.MESH,
        )

    def load(t):
        owner = lax.rem(me + 1 + t, n)
        return pltpu.make_async_copy(
            sketch_ref.at[pl.ds(owner * block, block)], rows_buf.at[t], load_sem.at[t]
        )

    barrier = pltpu.get_barrier_semaphore()
    for t in range(1, n):
        pl.semaphore_signal(
            barrier, inc=1, device_id={"dom": lax.rem(me + t, n)},
            device_id_type=pl.DeviceIdType.MESH,
        )
    for t in range(1, groups):
        pl.semaphore_signal(
            barrier, inc=1, device_id={"shift": lax.rem(group + t, groups)},
            device_id_type=pl.DeviceIdType.MESH,
        )
    arguments = [
        pltpu.make_async_copy(src_hbm, src_ref, in_sem.at[0]),
        pltpu.make_async_copy(kappa_hbm, kappa_ref, in_sem.at[1]),
        pltpu.make_async_copy(mass_hbm, mass_ref, in_sem.at[2]),
    ]
    for copy in arguments:
        copy.start()
    for t in range(n):
        load(t).start()
    for copy in arguments:
        copy.wait()
    pl.semaphore_wait(barrier, n - 1 + groups - 1)

    def sides(side):
        if side == 0:
            return slab - HALO, pl.ds(0, HALO), right
        return 0, pl.ds(slab + HALO, HALO), left

    def own_halo(side):
        first, target, there = sides(side)
        return remote(
            src_ref.at[:, pl.ds(first, HALO)], mine_ref.at[:, target],
            own_send.at[side], own_recv.at[side], dom=there,
        )

    hops = []
    for k in range(1, groups // 2 + 1):
        for way in range(2):
            parts = (0, nb)
            if 2 * k == groups:
                parts = ((0, nb // 2), (nb // 2, nb - nb // 2))[way]
            hops.append((way, k, pl.ds(*parts)))

    def shifted(way, k):
        step = k if way == 0 else groups - k
        return lax.rem(group + step, groups)

    def across(hop):
        way, k, part = hop
        if k == 1:
            slot, src = group, src_ref.at[part]
        else:
            slot = shifted(1 - way, k - 1)
            src = wide_ref.at[slot, part, pl.ds(HALO, slab)]
        return remote(
            src, wide_ref.at[slot, part, pl.ds(HALO, slab)],
            z_send.at[way, k - 1], z_recv.at[way, k - 1], shift=shifted(way, 1),
        )

    def halo(hop, side):
        way, k, part = hop
        slot = shifted(1 - way, k)
        first, target, there = sides(side)
        return remote(
            wide_ref.at[slot, part, pl.ds(HALO + first, HALO)], wide_ref.at[slot, part, target],
            halo_send.at[way, k - 1, side], halo_recv.at[way, k - 1, side], dom=there,
        )

    def coeff_halo(which, side):
        ref = (kappa_ref, mass_ref)[which]
        first, target, there = sides(side)
        return remote(
            ref.at[pl.ds(first, HALO)], coeff_ref.at[which, target], km_send.at[which, side],
            km_recv.at[which, side], dom=there,
        )

    @pl.when(has_right)
    def _():
        own_halo(0).start()
        for which in range(2):
            coeff_halo(which, 0).start()

    @pl.when(has_left)
    def _():
        own_halo(1).start()
        for which in range(2):
            coeff_halo(which, 1).start()

    for hop in hops:
        if hop[1] == 1:
            across(hop).start()

    mine_ref[:, pl.ds(HALO, slab)] = src_ref[...]
    coeff_ref[0, pl.ds(HALO, slab)] = kappa_ref[...]
    coeff_ref[1, pl.ds(HALO, slab)] = mass_ref[...]

    @pl.when(jnp.logical_not(has_left))
    def _():
        mine_ref[:, pl.ds(0, HALO)] = jnp.zeros(
            (nb, HALO) + src_ref.shape[2:], jnp.float32
        )
        coeff_ref[:, pl.ds(0, HALO)] = jnp.zeros((2, HALO) + src_ref.shape[2:], jnp.float32)

    @pl.when(jnp.logical_not(has_right))
    def _():
        mine_ref[:, pl.ds(slab + HALO, HALO)] = jnp.zeros(
            (nb, HALO) + src_ref.shape[2:], jnp.float32
        )
        coeff_ref[:, pl.ds(slab + HALO, HALO)] = jnp.zeros(
            (2, HALO) + src_ref.shape[2:], jnp.float32
        )

    @pl.when(has_left)
    def _():
        own_halo(0).wait_recv()
        for which in range(2):
            coeff_halo(which, 0).wait_recv()

    @pl.when(has_right)
    def _():
        own_halo(1).wait_recv()
        for which in range(2):
            coeff_halo(which, 1).wait_recv()

    keep = pltpu.make_async_copy(mine_ref, wide_ref.at[group], own_sem)
    keep.start()
    low, high = edge_flags()
    mass = coeff_ref[1]
    diag = (6.0 - coeff_ref[0]) + MID * mass
    planes = slab + 2 * HALO
    grid_tail = src_ref.shape[2:]
    mask1 = plane_mask((planes - 2,) + grid_tail, 2, low, high)
    mask2 = plane_mask((planes - 4,) + grid_tail, 1, low, high)

    def one_source(b, carry):
        fields = basis_fields(mine_ref[b], diag, mass, mask1, mask2)
        for k, field in enumerate(fields):
            rounded = field.astype(jnp.bfloat16)
            raw_ref[k * nb + b] = rounded
            raw_ref[columns + k * nb + b] = (field - rounded.astype(jnp.float32)).astype(
                jnp.bfloat16
            )
        return carry

    lax.fori_loop(0, nb, one_source, 0)
    fields_ref[...] = raw_ref[...].reshape(fields_ref.shape)

    def forward(hop):
        across(hop).wait_recv()
        for later in hops:
            if later[0] == hop[0] and later[1] == hop[1] + 1:
                across(later).start()

        @pl.when(has_right)
        def _():
            halo(hop, 0).start()

        @pl.when(has_left)
        def _():
            halo(hop, 1).start()

    early = [hop for hop in hops if hop[1] < groups // 2]
    late = [hop for hop in hops if hop[1] == groups // 2]
    def scatter(t):
        return remote(
            out_buf.at[t], in_buf.at[t], rs_send.at[t], rs_recv.at[t],
            dom=lax.rem(me + 1 + t, n),
        )

    per = next(size for size in (PIECES, 2, 1) if n % size == 0)

    def multiply(u):
        for t in range(per):
            load(u * per + t).wait()
        product = lax.dot_general(
            rows_buf[pl.ds(u * per, per)].reshape(per * block, fields_ref.shape[1]),
            fields_ref[...], (((1,), (1,)), ((), ())), preferred_element_type=jnp.float32,
        )
        turned = product.T
        summed = turned[:columns] + turned[columns:]
        return [summed[:, t * block : (t + 1) * block] for t in range(per)]

    def send(t, piece):
        out_buf[t] = piece
        scatter(t).start()

    def step(u, carry):
        for t, piece in enumerate(multiply(u)):
            send(u * per + t, piece)
        return carry

    lax.fori_loop(0, n // per - 1, step, 0)
    pieces = multiply(n // per - 1)
    for t in range(per - 1):
        send(n - per + t, pieces[t])
    total = pieces[per - 1]
    for hop in early:
        forward(hop)

    for t in range(n - 1):
        scatter(t).wait_recv()
        total = total + in_buf[t]

    lane = lax.broadcasted_iota(jnp.int32, (nb, LANES), 1)
    gram = jnp.zeros((nb, LANES), jnp.float32)
    for p, (i, k) in enumerate(PAIRS):
        value = jnp.sum(
            total[i * nb : (i + 1) * nb] * total[k * nb : (k + 1) * nb], axis=1, keepdims=True
        )
        gram = jnp.where(lane == p, value, gram)
    gram_own[...] = gram

    def share(t):
        return remote(
            gram_own, gram_in.at[t - 1], g_send.at[t - 1], g_recv.at[t - 1],
            dom=lax.rem(me + t, n),
        )

    for t in range(1, n):
        share(t).start()
    for t in range(1, n):
        share(t).wait_recv()
        gram = gram + gram_in[t - 1]
    gram_all[group] = gram
    for hop in late:
        forward(hop)

    def spread(t):
        return remote(
            gram_all.at[group], gram_all.at[group], s_send.at[t - 1], s_recv.at[t - 1],
            shift=lax.rem(group + t, groups),
        )

    for t in range(1, groups):
        spread(t).start()
    tau = jnp.zeros((1, LANES), jnp.float32)
    lane_row = lax.broadcasted_iota(jnp.int32, (1, LANES), 1)
    for j in range(ids_ref.shape[0]):
        tau = jnp.where(lane_row == j, table_ref[ids_ref[j]] - MID, tau)
    for t in range(1, groups):
        spread(t).wait_recv()
    count = groups * nb
    solved = coefficients(gram_all[...].reshape(count, LANES), tau)
    shifts = ids_ref.shape[0]
    packed = jnp.zeros((count, LANES), jnp.float32)
    lane_count = lax.broadcasted_iota(jnp.int32, (count, LANES), 1)
    for i in range(3):
        value = jnp.where(lane_count < shifts, solved[i], 0.0)
        packed = packed + (pltpu.roll(value, i * shifts, 1) if i else value)
    c_ref[...] = packed

    for hop in hops:
        @pl.when(has_left)
        def _():
            halo(hop, 0).wait_recv()

        @pl.when(has_right)
        def _():
            halo(hop, 1).wait_recv()

    keep.wait()

    @pl.when(has_right)
    def _():
        own_halo(0).wait_send()
        for hop in hops:
            halo(hop, 0).wait_send()
        for which in range(2):
            coeff_halo(which, 0).wait_send()

    @pl.when(has_left)
    def _():
        own_halo(1).wait_send()
        for hop in hops:
            halo(hop, 1).wait_send()
        for which in range(2):
            coeff_halo(which, 1).wait_send()

    for t in range(1, groups):
        spread(t).wait_send()
    for hop in hops:
        across(hop).wait_send()
    for t in range(n - 1):
        scatter(t).wait_send()
    for t in range(1, n):
        share(t).wait_send()


def combine_kernel(wide_ref, coeff_ref, c_ref, table_ref, ids_ref, sol_ref, res_ref, step_ref):
    batch, planes = wide_ref.shape[0], wide_ref.shape[1]
    me = lax.axis_index("dom")
    has_low, has_high = me > 0, me < lax.axis_size("dom") - 1
    shifts = ids_ref.shape[0]
    first = pl.program_id(0) * batch

    def inside(field, width):
        return jnp.concatenate(
            [
                jnp.where(has_low, field[:width], 0.0),
                field[width:-width],
                jnp.where(has_high, field[-width:], 0.0),
            ],
            axis=0,
        )

    @pl.when(pl.program_id(0) == 0)
    def _():
        for j in range(shifts):
            sigma = table_ref[ids_ref[j]]
            step_ref[j] = sigma * (coeff_ref[1, 1:-1] - 1.0) - coeff_ref[0, 1:-1]

    def one_source(i, carry):
        w0 = inside(wide_ref[i], HALO)
        own = w0[3:-3]
        near = neighbour_sum(w0)
        b = first + i
        for j in range(shifts):
            center = 6.0 + table_ref[ids_ref[j]]
            v1 = inside(step_ref[j] * w0[1:-1] - near, 2)
            v2 = inside(step_ref[j, 1:-1] * v1[1:-1] - neighbour_sum(v1), 1)
            v3 = step_ref[j, 2:-2] * v2[1:-1] - neighbour_sum(v2)
            v1, v2 = v1[2:-2], v2[1:-1]
            c0 = c_ref[b, j]
            c1 = c_ref[b, shifts + j] * (1.0 / 6.0)
            c2 = c_ref[b, 2 * shifts + j] * (1.0 / 36.0)
            sol_ref[j, i] = c0 * own + c1 * v1 + c2 * v2
            res_ref[j, i] = (
                (1.0 - c0 * center) * own - (c0 + c1 * center) * v1
                - (c1 + c2 * center) * v2 - c2 * v3
            )
        return carry

    lax.fori_loop(0, batch, one_source, 0)


def on_device(sources, kappa, mass, shift_table, shift_ids, sketch):
    n, groups = lax.axis_size("dom"), lax.axis_size("shift")
    nb, slab = sources.shape[0], sources.shape[1]
    tail = sources.shape[2:]
    shifts = shift_ids.shape[0]
    rows = sketch.shape[0]
    block = rows // n
    cells = slab * tail[0] * tail[1]
    planes = slab + 2 * HALO
    count = groups * nb
    columns = BASIS * nb
    vmem = pl.BlockSpec(memory_space=pltpu.VMEM)
    hbm = pl.BlockSpec(memory_space=pl.ANY)
    smem = pl.BlockSpec(memory_space=pltpu.SMEM)
    dma = pltpu.SemaphoreType.DMA
    f32 = jnp.float32
    wide, coeff, solved = pl.pallas_call(
        functools.partial(project_kernel, n, groups),
        out_shape=(
            jax.ShapeDtypeStruct((groups, nb, planes) + tail, f32),
            jax.ShapeDtypeStruct((2, planes) + tail, f32),
            jax.ShapeDtypeStruct((count, LANES), f32),
        ),
        in_specs=[hbm, hbm, hbm, smem, smem, hbm],
        out_specs=(hbm, vmem, vmem),
        scratch_shapes=[
            pltpu.VMEM(sources.shape, f32),
            pltpu.VMEM(kappa.shape, f32),
            pltpu.VMEM(mass.shape, f32),
            pltpu.VMEM((nb, planes) + tail, f32),
            pltpu.VMEM((n, block, slab) + tail, jnp.bfloat16),
            pltpu.VMEM((2 * columns, slab) + tail, jnp.bfloat16),
            pltpu.VMEM((2 * columns, cells), jnp.bfloat16),
            pltpu.VMEM((n - 1, columns, block), f32),
            pltpu.VMEM((n - 1, columns, block), f32),
            pltpu.VMEM((nb, LANES), f32),
            pltpu.VMEM((n - 1, nb, LANES), f32),
            pltpu.VMEM((groups, nb, LANES), f32),
            dma((n,)),
            dma((3,)), dma,
            dma((2,)), dma((2,)),
            dma((2, groups // 2)), dma((2, groups // 2)),
            dma((2, groups // 2, 2)), dma((2, groups // 2, 2)),
            dma((2, 2)), dma((2, 2)),
            dma((n - 1,)), dma((n - 1,)),
            dma((n - 1,)), dma((n - 1,)),
            dma((groups - 1,)), dma((groups - 1,)),
        ],
        compiler_params=pltpu.CompilerParams(
            collective_id=0, has_side_effects=True, vmem_limit_bytes=56 << 20
        ),
        name="project",
    )(sources, kappa, mass, shift_table, shift_ids, sketch)

    batch = 4 if count % 4 == 0 else 1
    out = jax.ShapeDtypeStruct((shifts, count, slab) + tail, f32)
    out_spec = pl.BlockSpec((shifts, batch, slab) + tail, lambda i: (0, i, 0, 0, 0))
    return pl.pallas_call(
        combine_kernel,
        grid=(count // batch,),
        out_shape=(out, out),
        in_specs=[
            pl.BlockSpec((batch, planes) + tail, lambda i: (i, 0, 0, 0)),
            pl.BlockSpec((2, planes) + tail, lambda i: (0, 0, 0, 0)),
            smem, smem, smem,
        ],
        out_specs=(out_spec, out_spec),
        scratch_shapes=[pltpu.VMEM((shifts, planes - 2) + tail, f32)],
        compiler_params=pltpu.CompilerParams(vmem_limit_bytes=63 << 20),
        name="combine",
    )(wide.reshape((count, planes) + tail), coeff, solved, shift_table, shift_ids)


def solution(mesh):
    placed = (
        P("shift", "dom", None, None),
        P("dom", None, None),
        P("dom", None, None),
        P(),
        P("shift"),
        P(None, "dom", None, None),
    )
    return jax.shard_map(
        on_device,
        mesh=mesh,
        in_specs=placed,
        out_specs=(P("shift", None, "dom", None, None), P("shift", None, "dom", None, None)),
        check_vma=False,
    )
```
